32 devices in a mesh: gx: 4 (over y, core), gy: 8 (over z, x).
Axes of the slice: x: 2, y: 2, z: 4, core: 2. Of those that a mesh axis runs over, the one named last changes fastest.
Arguments:
- hidden_states: bfloat16 [1024, 128], replicated, may hold values from -60 to 60
- item_table: bfloat16 [262144, 128], P(('gx', 'gy')), may hold values from -1.796875 to 1.796875
- targets: int32 [1024], replicated, may hold values from 0 to 262143
Outputs:
- expected: float32 [1024, 128], P(('gx', 'gy'))
- nll: float32 [1024], P(('gx', 'gy'))
The draws below stay inside these ranges and needn't reach their ends.
All inputs are finite; a program needn't handle non-finite values.
Results may differ from the reference program's by a relative error of at most 0.0023.
Values sent between devices are 32-bit elements; how exact they have to be, the bound alone decides.
A program may use at most 64 MiB of HBM per device.

```python
import jax
import jax.numpy as jnp
from jax import lax

D = 128
BLK = 512
P_SIZE = 1024
ITEMS = 262144


def draw_hidden_states(key, part):
    first_key = jax.random.fold_in(jax.random.fold_in(key, 17), 0)
    normal_draw = jax.random.normal(first_key, (P_SIZE, D), jnp.float32)
    result_rows = jnp.clip(normal_draw, -6.0, 6.0)
    return result_rows.astype(jnp.bfloat16)


def plant(entries, own_key, smallest, high):
    longest = entries.shape.index(max(entries.shape))
    spots = []
    for shift in (0, 1):
        where = [jax.random.randint(jax.random.fold_in(own_key, axis), (), 0, length) for axis, length in enumerate(entries.shape)]
        where[longest] = (where[longest] + shift) % entries.shape[longest]
        spots.append(tuple(where))
    return entries.at[spots[0]].set(smallest).at[spots[1]].set(high)


def shard_levels(stream_key, dims, shards, low, largest):
    def one(dim, shards_of):
        draws = jax.random.uniform(jax.random.fold_in(jax.random.fold_in(stream_key, 6), dim), (shards_of,), jnp.float32, low / len(shards), largest / len(shards))
        return jnp.repeat(jnp.exp(draws), dims[dim] // shards_of).reshape((-1,) + (1,) * (len(dims) - dim - 1))

    factor_of = one(*shards[0])
    for cut in shards[1:]:
        factor_of = factor_of * one(*cut)
    return factor_of


def normal_values(rng, dims, spread, limit, pieces=(), dtype=jnp.bfloat16):
    gain = shard_levels(rng, dims, pieces, -0.22, 0.18) if pieces else 1.0
    entries = jax.random.normal(rng, dims, jnp.float32) * spread * gain
    return jnp.minimum(jnp.maximum(entries, -limit), limit).astype(dtype)


def setup_inputs(seed: int = 0) -> dict:
    key_list = jax.random.split(jax.random.key(seed), 4)
    return {
        "hidden_states": draw_hidden_states(jax.random.fold_in(key_list[3], 71), 0),
        "item_table": normal_values(key_list[1], (ITEMS, D), 0.3, 1.796875, ((0, 32),)),
        "targets": plant(jax.random.randint(key_list[2], (P_SIZE,), 0, ITEMS), jax.random.fold_in(key_list[2], 1), 0, ITEMS - 1).astype(jnp.int32),
    }


def reference(hidden_states, item_table, targets):
    nblocks = item_table.shape[0] // BLK
    blocks = item_table.reshape(nblocks, BLK, D)

    def visit_block(carry, block):
        highest, totals, weighted = carry
        scores = lax.dot_general(hidden_states, block, (((1,), (1,)), ((), ())), preferred_element_type=jnp.float32)
        block_max = jnp.max(scores, axis=1)
        exponent = jnp.exp(scores - block_max[:, None])
        block_sum = jnp.sum(exponent, axis=1)
        probs_low = exponent.astype(jnp.bfloat16)
        block_acc = jnp.dot(probs_low, block, preferred_element_type=jnp.float32)
        new_max = jnp.maximum(highest, block_max)
        retain = jnp.exp(highest - new_max)
        rescale = jnp.exp(block_max - new_max)
        totals = totals * retain + block_sum * rescale
        weighted = weighted * retain[:, None] + block_acc * rescale[:, None]
        return (new_max, totals, weighted), None

    start_state = (jnp.full((P_SIZE,), -1e30, jnp.float32), jnp.zeros((P_SIZE,), jnp.float32), jnp.zeros((P_SIZE, D), jnp.float32))
    (highest, totals, weighted), unused_out = lax.scan(visit_block, start_state, blocks)
    target_rows = item_table[targets]
    target_logit = jnp.sum(hidden_states.astype(jnp.float32) * target_rows.astype(jnp.float32), axis=1)
    expected = weighted / totals[:, None]
    nll = highest + jnp.log(totals) - target_logit
    return expected, nll
```

```python
import functools

import jax
import jax.numpy as jnp
from jax import lax
from jax.experimental import pallas as pl
from jax.experimental.pallas import tpu as pltpu
from jax.sharding import PartitionSpec as P

AXES = ("gx", "gy")
CHUNK = 256
BLOCK = 1024
SUB = 256
MESH = pl.DeviceIdType.MESH
NT = (((1,), (1,)), ((), ()))


def kernel(n, ngy, rows, hid, tab, tgt, exp_out, nll_out,
           tabt, s_even, s_odd, acc, send, recv, send_sem, recv_sem):
    positions, width = hid.shape
    items = tab.shape[0]
    nchunk = positions // CHUNK
    nblock = items // BLOCK
    per_chunk = CHUNK // rows
    stat_row = send.shape[1] - 8
    gx = lax.axis_index("gx")
    gy = lax.axis_index("gy")
    me = gx * ngy + gy

    barrier = pltpu.get_barrier_semaphore()

    def greet(k, c):
        other = lax.rem(me + k, n)
        pl.semaphore_signal(barrier, inc=1, device_id=(other // ngy, lax.rem(other, ngy)), device_id_type=MESH)
        return c

    lax.fori_loop(1, n, greet, 0)

    eye = (lax.broadcasted_iota(jnp.int32, (width, width), 0)
           == lax.broadcasted_iota(jnp.int32, (width, width), 1)).astype(jnp.float32).astype(jnp.bfloat16)

    def turn(i, c):
        at = pl.ds(pl.multiple_of(i * SUB, SUB), SUB)
        tabt[0:width, at] = lax.dot_general(eye, tab[at, :], NT, preferred_element_type=jnp.float32).astype(jnp.bfloat16)
        return c

    lax.fori_loop(0, items // SUB, turn, 0, unroll=4)
    tabt[width:, :] = jnp.ones((tabt.shape[0] - width, items), jnp.bfloat16)

    first = me // per_chunk + 1
    sub_iota = lax.broadcasted_iota(jnp.int32, (8, CHUNK), 0)

    def chunk_of(k):
        return lax.rem(first + k, nchunk)

    def score(chunk, block, s_ref):
        at = pl.multiple_of(chunk * CHUNK, CHUNK)
        states = hid[pl.ds(at, CHUNK), :]
        top = jnp.full((8, CHUNK), -jnp.inf, jnp.float32)
        for sub in range(BLOCK // SUB):
            base = pl.multiple_of(block * BLOCK + sub * SUB, SUB)
            s = lax.dot_general(tab[pl.ds(base, SUB), :], states, NT, preferred_element_type=jnp.float32)
            s_ref[sub * SUB:(sub + 1) * SUB, :] = s
            for g in range(SUB // 8):
                top = jnp.maximum(top, s[8 * g:8 * g + 8])
        return jnp.max(top, axis=0, keepdims=True)

    def soft(block, s_ref, top, highest, place, hit):
        new = jnp.maximum(highest, top)
        retain = jnp.exp(highest - new)
        here = place - block * BLOCK
        parts = []
        for g in range(BLOCK // 8):
            s = s_ref[8 * g:8 * g + 8, :]
            hit = jnp.where(here == 8 * g, s, hit)
        p = jnp.exp(s_ref[...] - new).astype(jnp.bfloat16)
        base = pl.multiple_of(block * BLOCK, BLOCK)
        acc[...] = acc[...] * retain + jnp.dot(tabt[:, pl.ds(base, BLOCK)], p, preferred_element_type=jnp.float32)
        return new, hit

    def pair(k, place, j, carry):
        top_even, highest, hit = carry
        chunk = chunk_of(k)
        top_odd = score(chunk, 2 * j + 1, s_odd)
        highest, hit = soft(2 * j, s_even, top_even, highest, place, hit)
        later = k * nblock + 2 * j + 2
        top_even = score(chunk_of(later // nblock), lax.rem(later, nblock), s_even)
        highest, hit = soft(2 * j + 1, s_odd, top_odd, highest, place, hit)
        return top_even, highest, hit

    def one_chunk(k, top_even):
        chunk = chunk_of(k)
        at = pl.multiple_of(chunk * CHUNK, CHUNK)
        place = tgt[0:1, pl.ds(at, CHUNK)] - me * items - sub_iota
        acc[...] = jnp.zeros_like(acc)
        top_even, highest, hit = lax.fori_loop(
            0, nblock // 2, functools.partial(pair, k, place),
            (top_even, jnp.full((1, CHUNK), -1e30, jnp.float32), jnp.zeros((8, CHUNK), jnp.float32)))
        weighted = acc[0:width, :].T
        stats = jnp.concatenate(
            [highest, acc[width:width + 1, :], jnp.sum(hit, axis=0, keepdims=True), jnp.zeros((5, CHUNK), jnp.float32)], axis=0)
        for o in range(per_chunk):
            owner = chunk * per_chunk + o
            send[owner, 0:rows, :] = weighted[o * rows:(o + 1) * rows, :]
            turned = stats if o == 0 else pltpu.roll(stats, CHUNK - o * rows, 1)
            send[owner, stat_row:, :] = turned[:, 0:width]
        for o in range(per_chunk):
            owner = chunk * per_chunk + o

            @pl.when(owner != me)
            def _():
                slot = lax.rem(me - owner - 1 + n, n)
                pltpu.make_async_remote_copy(
                    src_ref=send.at[owner], dst_ref=recv.at[slot], send_sem=send_sem, recv_sem=recv_sem,
                    device_id=(owner // ngy, lax.rem(owner, ngy)), device_id_type=MESH).start()
        return top_even

    top_even = score(chunk_of(0), 0, s_even)
    pl.semaphore_wait(barrier, n - 1)
    lax.fori_loop(0, nchunk, one_chunk, top_even)

    recv[n - 1] = send[me]
    most = recv.at[pl.ds(0, n - 1)]
    whole = pltpu.make_async_remote_copy(
        src_ref=most, dst_ref=most, send_sem=send_sem, recv_sem=recv_sem,
        device_id=(gx, gy), device_id_type=MESH)
    whole.wait_send()
    whole.wait_recv()

    tops = recv[:, stat_row, :]
    top = jnp.max(tops, axis=0, keepdims=True)
    factor = jnp.exp(tops - top)
    total = jnp.sum(factor * recv[:, stat_row + 1, :], axis=0, keepdims=True)
    target = jnp.sum(recv[:, stat_row + 2, :], axis=0, keepdims=True)
    nll_out[...] = top + jnp.log(total) - target
    share = (factor / total).T
    out = jnp.zeros((rows, width), jnp.float32)
    for s in range(n):
        out = out + share[0:rows, s:s + 1] * recv[s, 0:rows, :]
    exp_out[...] = out


def solution(mesh):
    n = mesh.size
    ngy = mesh.shape["gy"]

    def local(hidden_states, item_table, targets):
        positions, width = hidden_states.shape
        items = item_table.shape[0]
        rows = positions // n
        held = -(-rows // 8) * 8 + 8
        vmem = pl.BlockSpec(memory_space=pltpu.VMEM)
        expected, nll = pl.pallas_call(
            functools.partial(kernel, n, ngy, rows),
            out_shape=(jax.ShapeDtypeStruct((rows, width), jnp.float32), jax.ShapeDtypeStruct((1, width), jnp.float32)),
            in_specs=[vmem, vmem, vmem],
            out_specs=(vmem, vmem),
            scratch_shapes=[
                pltpu.VMEM((width + 16, items), jnp.bfloat16),
                pltpu.VMEM((BLOCK, CHUNK), jnp.float32),
                pltpu.VMEM((BLOCK, CHUNK), jnp.float32),
                pltpu.VMEM((width + 16, CHUNK), jnp.float32),
                pltpu.VMEM((n, held, width), jnp.float32),
                pltpu.VMEM((n, held, width), jnp.float32),
                pltpu.SemaphoreType.DMA,
                pltpu.SemaphoreType.DMA,
            ],
            compiler_params=pltpu.CompilerParams(collective_id=0, has_side_effects=True, vmem_limit_bytes=60000000),
        )(hidden_states, item_table, targets.reshape(1, positions))
        return expected, nll[0, :rows]

    return jax.shard_map(
        local, mesh=mesh,
        in_specs=(P(), P(AXES, None), P()),
        out_specs=(P(AXES, None), P(AXES)),
        check_vma=False,
    )
```

```python
import functools

import jax
import jax.numpy as jnp
from jax import lax
from jax.experimental import pallas as pl
from jax.experimental.pallas import tpu as pltpu
from jax.sharding import PartitionSpec as P

AXES = ("gx", "gy")
BLOCK = 4096
SUB = 256
PARTS = 8
DEPTH = 512
MESH = pl.DeviceIdType.MESH
NT = (((1,), (1,)), ((), ()))


def kernel(ngx, ngy, rows, hid, table, tgt, packed,
           tab, tabt, held, acc, give, take, send, recv, give_sem, take_sem, send_sem, recv_sem, load_sem):
    CHUNK = rows * ngy
    positions, width = hid.shape
    items = table.shape[0]
    part = items // PARTS
    loads = []
    for i in range(PARTS):
        at = pl.ds(i * part, part)
        loads.append(pltpu.make_async_copy(table.at[at], tab.at[at], load_sem.at[i]))
        loads[i].start()
    nchunk = positions // CHUNK
    nblock = items // BLOCK
    stat_row = send.shape[1] - 8
    gx = lax.axis_index("gx")
    gy = lax.axis_index("gy")
    me = gx * ngy + gy
    core, line = lax.rem(gx, 2), gx // 2
    half = ngx // 2 * ngy
    place_of_me = line * ngy + gy
    partner = (gx + 1 - 2 * core, gy)

    barrier = pltpu.get_barrier_semaphore()

    def greet(k, c):
        other = lax.rem(place_of_me + k, half)
        pl.semaphore_signal(barrier, inc=1, device_id=(other // ngy * 2 + core, lax.rem(other, ngy)), device_id_type=MESH)
        return c

    lax.fori_loop(1, half, greet, 0)
    pl.semaphore_signal(barrier, inc=1, device_id=partner, device_id_type=MESH)

    def turn(base, count):
        at = pl.ds(base, count)
        tabt[0:width, at] = tab[at, :].T

    tabt[width:, :] = jnp.ones((tabt.shape[0] - width, items), jnp.bfloat16)

    sub_iota = lax.broadcasted_iota(jnp.int32, (8, CHUNK), 0)

    def chunk_of(k):
        mine = lax.rem(k, 2)
        return lax.rem(line + 1 + k // 2, nchunk // 2) * 2 + mine * core + (1 - mine) * (1 - core)

    def score(chunk, block, sub):
        at = pl.multiple_of(chunk * CHUNK, CHUNK)
        base = pl.multiple_of(block * BLOCK + sub * SUB, SUB)
        s = lax.dot_general(tab[pl.ds(base, SUB), :], hid[pl.ds(at, CHUNK), :], NT, preferred_element_type=jnp.float32)
        held[sub * SUB:(sub + 1) * SUB, :] = s
        return functools.reduce(jnp.maximum, [s[8 * g:8 * g + 8] for g in range(SUB // 8)])

    def top_of(tops):
        return jnp.max(functools.reduce(jnp.maximum, tops), axis=0, keepdims=True)

    def step(k, place, turning, j, carry):
        top, highest, hit = carry
        new = jnp.maximum(highest, top)
        retain = jnp.exp(highest - new)
        here = place - j * BLOCK
        later = k * nblock + j + 1
        chunk, block = chunk_of(later // nblock), lax.rem(later, nblock)
        tops, added = [], None
        for q in range(BLOCK // DEPTH):
            base = pl.multiple_of(j * BLOCK + q * DEPTH, DEPTH)
            if turning:
                turn(base, DEPTH)
            s = held[q * DEPTH:(q + 1) * DEPTH, :]
            for g in range(DEPTH // 8):
                hit = jnp.where(here == q * DEPTH + 8 * g, s[8 * g:8 * g + 8], hit)
            p = jnp.exp(s - new).astype(jnp.bfloat16)
            part = jnp.dot(tabt[:, pl.ds(base, DEPTH)], p, preferred_element_type=jnp.float32)
            added = part if added is None else added + part
            for sub in range(q * DEPTH // SUB, (q + 1) * DEPTH // SUB):
                tops.append(score(chunk, block, sub))
        acc[...] = acc[...] * retain + added
        return top_of(tops), new, hit

    def one_chunk(turning, k, top):
        chunk = chunk_of(k)
        at = pl.multiple_of(chunk * CHUNK, CHUNK)
        place = tgt[0:1, pl.ds(at, CHUNK)] - me * items - sub_iota
        acc[...] = jnp.zeros_like(acc)
        top, highest, hit = lax.fori_loop(
            0, nblock, functools.partial(step, k, place, turning),
            (top, jnp.full((1, CHUNK), -1e30, jnp.float32), jnp.zeros((8, CHUNK), jnp.float32)))
        return top, highest, jnp.sum(hit, axis=0, keepdims=True)

    def passing(k):
        return pltpu.make_async_remote_copy(
            src_ref=give.at[k // 2], dst_ref=take.at[k // 2], send_sem=give_sem.at[k // 2], recv_sem=take_sem.at[k // 2],
            device_id=partner, device_id_type=MESH)

    def two_chunks(turning, kk, top):
        top, highest, hit = one_chunk(turning, 2 * kk, top)
        give[kk, 0:width + 8, :] = acc[0:width + 8, :]
        give[kk, width + 8:, :] = jnp.concatenate([highest, hit, jnp.zeros((6, CHUNK), jnp.float32)], axis=0)
        passing(2 * kk).start()
        top, highest, hit = one_chunk(False, 2 * kk + 1, top)
        passing(2 * kk).wait_recv()
        other = take[kk, width + 8:width + 9, :]
        both = jnp.maximum(highest, other)
        own_share, other_share = jnp.exp(highest - both), jnp.exp(other - both)
        weighted = (acc[0:width, :] * own_share + take[kk, 0:width, :] * other_share).T
        total = acc[width:width + 1, :] * own_share + take[kk, width:width + 1, :] * other_share
        stats = jnp.concatenate(
            [both, total, hit + take[kk, width + 9:width + 10, :], jnp.zeros((5, CHUNK), jnp.float32)], axis=0)
        chunk = chunk_of(2 * kk + 1)
        for o in range(ngy):
            owner = chunk // 2 * ngy + o
            send[owner, 0:rows, :] = weighted[o * rows:(o + 1) * rows, :]
            turned = stats if o == 0 else pltpu.roll(stats, CHUNK - o * rows, 1)
            send[owner, stat_row:, :] = turned[:, 0:width]
        for o in range(ngy):
            owner = chunk // 2 * ngy + o

            @pl.when(owner != place_of_me)
            def _():
                slot = lax.rem(place_of_me - owner - 1 + half, half)
                pltpu.make_async_remote_copy(
                    src_ref=send.at[owner], dst_ref=recv.at[slot], send_sem=send_sem, recv_sem=recv_sem,
                    device_id=(chunk, o), device_id_type=MESH).start()
        return top

    tops = []
    for i in range(PARTS):
        loads[i].wait()
        tops += [score(chunk_of(0), 0, sub) for sub in range(BLOCK // SUB) if sub * SUB // part == i]
    top = top_of(tops)
    pl.semaphore_wait(barrier, half)
    top = two_chunks(True, 0, top)
    lax.fori_loop(1, nchunk // 2, functools.partial(two_chunks, False), top)

    def given(kk, c):
        passing(2 * kk).wait_send()
        return c

    lax.fori_loop(0, nchunk // 2, given, 0)
    recv[half - 1] = send[place_of_me]
    most = recv.at[pl.ds(0, half - 1)]
    whole = pltpu.make_async_remote_copy(
        src_ref=most, dst_ref=most, send_sem=send_sem, recv_sem=recv_sem,
        device_id=(gx, gy), device_id_type=MESH)
    whole.wait_send()
    whole.wait_recv()

    tops = recv[:, stat_row, :]
    top = jnp.max(tops, axis=0, keepdims=True)
    factor = jnp.exp(tops - top)
    total = jnp.sum(factor * recv[:, stat_row + 1, :], axis=0, keepdims=True)
    target = jnp.sum(recv[:, stat_row + 2, :], axis=0, keepdims=True)
    packed[stat_row:stat_row + 1, :] = top + jnp.log(total) - target
    share = (factor / total).T
    out = jnp.zeros((rows, width), jnp.float32)
    for s in range(half):
        out = out + share[0:rows, s:s + 1] * recv[s, 0:rows, :]
    packed[0:rows, :] = out


def unpack(rows, stat_row, packed, exp_out, nll_out):
    exp_out[...] = packed[0:rows, :]
    nll_out[...] = packed[stat_row, 0:rows]


def solution(mesh):
    n = mesh.size
    ngx, ngy = mesh.shape["gx"], mesh.shape["gy"]

    def local(hidden_states, item_table, targets):
        positions, width = hidden_states.shape
        items = item_table.shape[0]
        rows = positions // n
        chunk = rows * ngy
        tall = -(-rows // 8) * 8 + 8
        vmem = pl.BlockSpec(memory_space=pltpu.VMEM)
        packed = pl.pallas_call(
            functools.partial(kernel, ngx, ngy, rows),
            out_shape=jax.ShapeDtypeStruct((tall, width), jnp.float32),
            in_specs=[vmem, pl.BlockSpec(memory_space=pl.ANY), vmem],
            out_specs=vmem,
            scratch_shapes=[
                pltpu.VMEM((items, width), jnp.bfloat16),
                pltpu.VMEM((width + 16, items), jnp.bfloat16),
                pltpu.VMEM((BLOCK, chunk), jnp.float32),
                pltpu.VMEM((width + 16, chunk), jnp.float32),
                pltpu.VMEM((ngx // 2, width + 16, chunk), jnp.float32),
                pltpu.VMEM((ngx // 2, width + 16, chunk), jnp.float32),
                pltpu.VMEM((n // 2, tall, width), jnp.float32),
                pltpu.VMEM((n // 2, tall, width), jnp.float32),
                pltpu.SemaphoreType.DMA((ngx // 2,)),
                pltpu.SemaphoreType.DMA((ngx // 2,)),
                pltpu.SemaphoreType.DMA,
                pltpu.SemaphoreType.DMA,
                pltpu.SemaphoreType.DMA((PARTS,)),
            ],
            compiler_params=pltpu.CompilerParams(collective_id=0, has_side_effects=True, vmem_limit_bytes=60000000),
        )(hidden_states, item_table, targets.reshape(1, positions))
        return pl.pallas_call(
            functools.partial(unpack, rows, tall - 8),
            out_shape=(jax.ShapeDtypeStruct((rows, width), jnp.float32), jax.ShapeDtypeStruct((rows,), jnp.float32)),
            in_specs=[vmem], out_specs=(vmem, vmem),
        )(packed)

    return jax.shard_map(
        local, mesh=mesh,
        in_specs=(P(), P(AXES, None), P()),
        out_specs=(P(AXES, None), P(AXES)),
        check_vma=False,
    )
```
